32 devices in a mesh: pts: 16 (over z, y, x), bev: 2 (over core).
Axes of the slice: x: 2, y: 2, z: 4, core: 2. Of those that a mesh axis runs over, the one named last changes fastest.
Arguments:
- point_feats: float32 [4, 131072], P(None, ('pts', 'bev')), may hold values from -6 to 6
- point_class: int32 [131072], P(('pts', 'bev')), may hold values from 0 to 10
- point_band: int32 [131072], P(('pts', 'bev')), may hold values from 0 to 1
- point_pillar: int32 [131072], P(('pts', 'bev')), may hold values from 0 to 1499
- point_counts: int32 [16], replicated, may hold values from 2048 to 8192
- pillar_cell: int32 [16, 2, 1500], P('pts', 'bev'), may hold values from 0 to 107135, as said below
- class_scores: float32 [11, 11], replicated, may hold values from 0 to 1
- encoder_weight: float32 [64, 15], replicated, may hold values from -1.5 to 1.5
- encoder_bias: float32 [64], replicated, may hold values from -3 to 3
Outputs:
- bev_image: bfloat16 [16, 64, 496, 432], P('pts', None, 'bev')
- class_counts: float32 [11], replicated
The draws below stay inside these ranges and needn't reach their ends.
Inputs may be any that keep to these rules, and one draw needn't show every extreme that they name: `pillar_cell`: for each frame and band the 1500 cells are distinct.
All inputs are finite; a program needn't handle non-finite values.
Results may differ from the reference program's by a relative error of at most 0.0033.
Values may be sent and summed in bfloat16 or wider, within the bound.
No kernel may reach another device: no remote copies, remote signals or barrier semaphores. Data moves between devices by JAX's collectives and lax.ppermute only.
A program may use at most 128 MiB of HBM per device.

```python
import jax
import jax.numpy as jnp
from jax import lax

C = 64
ROWS = 496
COLS = 432
CLASSES = 11
PIL_BAND = 1500
PTS_DEV = 4096
FRAMES = 16
BANDS = 2
BAND_ROWS = 248
FRAME_PTS = 8192
POINTS = 131072


def draw_pillar_cell(key, part):
    keys = jax.random.split(jax.random.fold_in(key, 7), FRAMES * BANDS)

    def choose(single):
        return jax.random.permutation(single, BAND_ROWS * COLS)[:PIL_BAND]
    return jax.vmap(choose)(keys).reshape(FRAMES, BANDS, PIL_BAND).astype(jnp.int32)


def draw_point_class(key, part):
    base = jax.random.fold_in(key, 11)
    dominant = jax.random.randint(jax.random.fold_in(base, 1), (FRAMES, 1), 0, CLASSES)
    picker = jax.random.randint(jax.random.fold_in(base, 2), (FRAMES, FRAME_PTS), 0, 2)
    others = jax.random.randint(jax.random.fold_in(base, 3), (FRAMES, FRAME_PTS), 0, CLASSES)
    chosen = jnp.where(picker == 0, dominant, others)
    return chosen.reshape(-1).astype(jnp.int32)


def touch_ends(array, rng, smallest, high):
    shape = array.shape
    index_at = [jax.random.randint(jax.random.fold_in(rng, axis), (), 0, shape[axis]) for axis in range(len(shape))]
    array = array.at[tuple(index_at)].set(smallest)
    longest = shape.index(max(shape))
    index_at[longest] = (index_at[longest] + 1) % shape[longest]
    return array.at[tuple(index_at)].set(high)


def block_scale(stream_key, dims, shards, smallest, top_value):
    def one(dim, blocks):
        heights = jax.random.uniform(jax.random.fold_in(jax.random.fold_in(stream_key, 6), dim), (blocks,), jnp.float32, smallest / len(shards), top_value / len(shards))
        return jnp.repeat(jnp.exp(heights), dims[dim] // blocks).reshape((-1,) + (1,) * (len(dims) - dim - 1))

    gain = one(*shards[0])
    for cut in shards[1:]:
        gain = gain * one(*cut)
    return gain


def scatter_about(stream_key, shape, scale, most, shards=(), kind=jnp.bfloat16):
    result = jax.random.normal(stream_key, shape, jnp.float32) * scale
    if len(shards) > 0:
        result = block_scale(stream_key, shape, shards, -0.22, 0.18) * result
    return jnp.clip(result, min=-most, max=most).astype(kind)


def setup_inputs(seed: int = 0) -> dict:
    key_list = jax.random.split(jax.random.key(seed), 10)
    return {
        "point_feats": scatter_about(key_list[0], (4, POINTS), 1.0, 6.0, ((1, 32),), jnp.float32),
        "point_class": draw_point_class(jax.random.fold_in(key_list[9], 71), 0),
        "point_band": touch_ends(jax.random.randint(key_list[2], (POINTS,), 0, BANDS), jax.random.fold_in(key_list[2], 1), 0, BANDS - 1).astype(jnp.int32),
        "point_pillar": touch_ends(jax.random.randint(key_list[3], (POINTS,), 0, PIL_BAND), jax.random.fold_in(key_list[3], 1), 0, PIL_BAND - 1).astype(jnp.int32),
        "point_counts": touch_ends(jax.random.randint(key_list[4], (FRAMES,), FRAME_PTS // 4, FRAME_PTS + 1), jax.random.fold_in(key_list[4], 1), FRAME_PTS // 4, FRAME_PTS).astype(jnp.int32),
        "pillar_cell": draw_pillar_cell(jax.random.fold_in(key_list[9], 71), 0),
        "class_scores": jnp.clip(jax.random.uniform(key_list[6], (CLASSES, CLASSES), jnp.float32, 0.0, 1.0), 0.0, 1.0),
        "encoder_weight": scatter_about(key_list[7], (C, 4 + CLASSES), (4 + CLASSES) ** -0.5, 1.5, (), jnp.float32),
        "encoder_bias": scatter_about(key_list[8], (C,), 0.5, 3.0, (), jnp.float32),
    }


def encode(raw_values, classes, class_scores, encoder_weight, encoder_bias):
    point_total = classes.shape[0]
    labels = lax.broadcasted_iota(jnp.int32, (class_scores.shape[1], point_total), 0)
    one_hot = (labels == classes[None, :]).astype(jnp.float32)
    painted = jnp.dot(class_scores, one_hot, precision=lax.Precision.HIGHEST)
    inputs = jnp.concatenate([raw_values, painted], axis=0)
    hidden = jnp.dot(encoder_weight, inputs, precision=lax.Precision.HIGHEST) + encoder_bias[:, None]
    return jnp.maximum(hidden, 0.0).astype(jnp.bfloat16)


def reference(point_feats, point_class, point_band, point_pillar, point_counts, pillar_cell, class_scores, encoder_weight, encoder_bias):
    feats = point_feats.reshape(4, FRAMES, FRAME_PTS).transpose(1, 0, 2)
    classes = point_class.reshape(FRAMES, FRAME_PTS)
    bands = point_band.reshape(FRAMES, FRAME_PTS)
    pillars = point_pillar.reshape(FRAMES, FRAME_PTS)
    position = lax.broadcasted_iota(jnp.int32, (FRAMES, FRAME_PTS), 1)
    is_valid = position < point_counts[:, None]

    def per_frame(pieces):
        frame_raw, labels, frame_bands, frame_pillars, is_live, frame_cells = pieces
        encoded = encode(frame_raw, labels, class_scores, encoder_weight, encoder_bias)
        segment_ids = jnp.where(is_live, frame_bands * PIL_BAND + frame_pillars, BANDS * PIL_BAND)
        pillar_sums = jax.ops.segment_sum(encoded.astype(jnp.float32).T, segment_ids, num_segments=BANDS * PIL_BAND + 1)[:-1]
        counts = jax.ops.segment_sum(jnp.ones(segment_ids.shape, jnp.float32), segment_ids, num_segments=BANDS * PIL_BAND + 1)[:-1]
        pillar_mean = (pillar_sums / jnp.maximum(counts, 1.0)[:, None]).astype(jnp.bfloat16)
        cell_base = BAND_ROWS * COLS * lax.broadcasted_iota(jnp.int32, (BANDS, PIL_BAND), 0)
        flat_cells = (frame_cells + cell_base).reshape(-1)
        bev_grid = jnp.zeros((C, ROWS * COLS), jnp.bfloat16).at[:, flat_cells].set(pillar_mean.T)
        return bev_grid.reshape(C, ROWS, COLS)

    bev_image = lax.map(per_frame, (feats, classes, bands, pillars, is_valid, pillar_cell))
    live_classes = jnp.where(is_valid, classes, CLASSES).reshape(-1)
    class_ids = lax.broadcasted_iota(jnp.int32, (CLASSES, 1), 0)
    class_tally = jnp.sum((class_ids == live_classes[None, :]).astype(jnp.float32), axis=1)
    class_counts = class_tally / PTS_DEV
    return bev_image, class_counts
```

```python
import jax
import jax.numpy as jnp
from jax import lax
from jax.experimental import pallas as pl
from jax.experimental.pallas import tpu as pltpu
from jax.sharding import PartitionSpec as P

ROWS = 496
COLS = 432
CLASSES = 11

LO = 256
STEP = 16
BUCKETS = 32
HIGHEST = lax.Precision.HIGHEST
NT = (((1,), (1,)), ((), ()))


def round_up(value, unit):
    return -(-value // unit) * unit


def iota(shape, axis):
    return lax.broadcasted_iota(jnp.int32, shape, axis)


def to_f32(mask):
    return jnp.where(mask, 1.0, 0.0).astype(jnp.float32)


def split3(value):
    high = value.astype(jnp.bfloat16).astype(jnp.float32)
    rest = value - high
    mid = rest.astype(jnp.bfloat16).astype(jnp.float32)
    return high, mid, rest - mid


def encoder_matrix(weight, scores, bias_row):
    channels, columns = weight.shape
    lane = iota((columns, 80), 1)
    row = iota((columns, 80), 0)
    pick = to_f32((lane < 24) & ((lane & 3) == row))
    shift = to_f32(iota((columns, CLASSES), 0) == iota((columns, CLASSES), 1) + 4)
    place_lane = iota((CLASSES, 80), 1)
    place = to_f32((place_lane >= 32) & ((place_lane & 15) == iota((CLASSES, 80), 0)))
    spread = jnp.dot(
        jnp.dot(shift, scores, precision=HIGHEST, preferred_element_type=jnp.float32),
        place,
        precision=HIGHEST,
        preferred_element_type=jnp.float32,
    )
    matrix = jnp.dot(
        weight, pick + spread, precision=HIGHEST, preferred_element_type=jnp.float32
    )
    eye = iota((channels, channels), 0) == iota((channels, channels), 1)
    bias = jnp.sum(jnp.where(eye, bias_row, 0.0), axis=1, keepdims=True)
    out_lane = iota((channels, 80), 1)
    matrix = matrix + jnp.where((out_lane >= 32) & ((out_lane & 15) == CLASSES), bias, 0.0)
    high, mid, low = split3(matrix)
    take_mid = ((out_lane >= 8) & (out_lane < 16)) | ((out_lane >= 48) & (out_lane < 64))
    take_low = ((out_lane >= 16) & (out_lane < 20)) | (out_lane >= 64)
    return jnp.where(take_mid, mid, jnp.where(take_low, low, high)).astype(jnp.bfloat16)


def two_level(values, hi, lo, hi_count):
    rows, total = values.shape
    tall = [values * to_f32(hi == h).astype(jnp.bfloat16) for h in range(hi_count)]
    one_hot = to_f32(iota((LO, total), 0) == lo).astype(jnp.bfloat16)
    return tall, one_hot


def pool_body(
    parts, spans, pillars, sub_of, *refs
):
    point_refs = refs[: 4 * parts]
    counts_ref, cell_ref, scores_ref, weight_ref, bias_ref = refs[4 * parts : 4 * parts + 5]
    sorted_ref, starts_ref, tally_ref = refs[4 * parts + 5 : 4 * parts + 8]
    cell_pad = refs[4 * parts + 8]
    frame = lax.axis_index("pts")
    band = lax.axis_index("bev")
    live_total = counts_ref[frame]
    channels = weight_ref.shape[0]
    hi_count = round_up(pillars, LO) // LO
    width = hi_count * LO

    matrix = encoder_matrix(weight_ref[...], scores_ref[...], bias_ref[...])
    sums = jnp.zeros((hi_count * channels + 16, LO), jnp.float32)
    tally = jnp.zeros((16, 1), jnp.float32)
    for part in range(parts):
        feats, classes, bands, pillar = [r[...] for r in point_refs[4 * part : 4 * part + 4]]
        feats = feats.reshape(feats.shape[-2:])
        classes = classes.reshape(1, -1)
        bands = bands.reshape(1, -1)
        pillar = pillar.reshape(1, -1)
        total = feats.shape[1]
        position = spans[part](band) * total + iota((1, total), 1)
        live = position < live_total
        live_class = jnp.where(live, classes, CLASSES)
        one_hot = to_f32(iota((16, total), 0) == live_class)
        tally = tally + jnp.sum(one_hot, axis=1, keepdims=True)
        one_hot = jnp.where(iota((16, total), 0) == CLASSES, 1.0, one_hot)
        high, mid, low = split3(jnp.concatenate([feats, feats], axis=0))
        top = iota((8, total), 0) < 4
        first = jnp.where(top, high, mid)
        third = jnp.where(top, high, low)
        stacked = jnp.concatenate(
            [first, first, third, jnp.zeros_like(first), one_hot, one_hot, one_hot], axis=0
        ).astype(jnp.bfloat16)
        hidden = jnp.dot(matrix, stacked, preferred_element_type=jnp.float32)
        encoded = jnp.maximum(hidden, 0.0).astype(jnp.bfloat16)
        hi = jnp.where(live & (bands == band), pillar >> 8, 15)
        lo = pillar & (LO - 1)
        tall, lo_hot = two_level(encoded, hi, lo, hi_count)
        tall.append(to_f32(iota((16, total), 0) == hi).astype(jnp.bfloat16))
        sums = sums + lax.dot_general(
            jnp.concatenate(tall, axis=0), lo_hot, NT, preferred_element_type=jnp.float32
        )
    diagonal = iota((16, 128), 0) == iota((16, 128), 1)
    tally_ref[...] = jnp.sum(jnp.where(diagonal, tally, 0.0), axis=0, keepdims=True)

    cell_pad[...] = jnp.full(cell_pad.shape, -1, jnp.int32)
    cell_pad[:, :pillars] = cell_ref[...].reshape(1, pillars)
    cell = cell_pad[...]
    cell_f = cell.astype(jnp.float32)
    grid_row = jnp.floor((cell_f + 0.5) * (1.0 / COLS)).astype(jnp.int32)
    grid_col = cell - grid_row * COLS
    sub, lane = (grid_col, grid_row) if sub_of == "col" else (grid_row, grid_col)
    block = jnp.where(cell >= 0, sub >> 4, BUCKETS - 1)
    member = to_f32(iota((BUCKETS, width), 0) == block)
    before = to_f32(iota((LO, LO), 0) < iota((LO, LO), 1)).astype(jnp.bfloat16)
    offset = jnp.zeros((BUCKETS, 1), jnp.float32)
    ranks = []
    for h in range(hi_count):
        chunk = member[:, h * LO : (h + 1) * LO]
        prefix = jnp.dot(
            chunk.astype(jnp.bfloat16), before, preferred_element_type=jnp.float32
        )
        ranks.append(prefix + offset)
        offset = offset + jnp.sum(chunk, axis=1, keepdims=True)
    square = iota((BUCKETS, 128), 0)
    across = iota((BUCKETS, 128), 1)
    starts_row = jnp.sum(jnp.where(square < across, offset, 0.0), axis=0, keepdims=True)
    starts_ref[...] = starts_row.astype(jnp.int32)
    start = jnp.sum(jnp.where(square == across, starts_row, 0.0), axis=1, keepdims=True)
    placed = jnp.zeros((hi_count * (channels + 16), LO), jnp.float32)
    extra = iota((16, LO), 0)
    counts = sums[hi_count * channels :]
    for h in range(hi_count):
        at = slice(h * LO, (h + 1) * LO)
        rank = jnp.sum(member[:, at] * (ranks[h] + start), axis=0, keepdims=True).astype(jnp.int32)
        mean = sums[h * channels : (h + 1) * channels] / jnp.maximum(counts[h : h + 1], 1.0)
        sub_h = sub[:, at]
        lane_h = lane[:, at]
        where = jnp.where(
            extra == 0,
            block[:, at],
            jnp.where(
                extra == 1,
                sub_h & (STEP - 1),
                jnp.where(extra == 2, lane_h >> 8, jnp.where(extra == 3, lane_h & 255, 0)),
            ),
        ).astype(jnp.float32)
        values = jnp.concatenate([mean, where], axis=0).astype(jnp.bfloat16)
        tall, lo_hot = two_level(values, rank >> 8, rank & (LO - 1), hi_count)
        placed = placed + lax.dot_general(
            jnp.concatenate(tall, axis=0), lo_hot, NT, preferred_element_type=jnp.float32
        )
    rows = channels + 16
    tail = iota((8, LO), 0)
    for h in range(hi_count):
        at = slice(h * LO, (h + 1) * LO)
        piece = placed[h * rows : (h + 1) * rows]
        sorted_ref[:channels, at] = piece[:channels]
        sub_s = piece[channels : channels + 1] * STEP + piece[channels + 1 : channels + 2]
        lane_s = piece[channels + 2 : channels + 3] * 256.0 + piece[channels + 3 : channels + 4]
        sorted_ref[channels:, at] = jnp.where(tail == 0, sub_s, jnp.where(tail == 1, lane_s, 0.0))
    sorted_ref[:, width:] = jnp.full((channels + 8, LO), 0.0, jnp.float32)
    sorted_ref[channels:, width:] = jnp.full((8, LO), -1.0, jnp.float32)


def place_body(first_block, starts_ref, sorted_ref, out_ref, acc_ref):
    block = pl.program_id(0) + first_block
    channels, step, lanes = out_ref.shape
    wide = round_up(lanes, 128)
    begin = starts_ref[0, block]
    end = starts_ref[0, block + 1]
    base = (begin >> 7) << 7
    turns = (end - base + LO - 1) // LO

    def partial(turn):
        at = pl.ds(pl.multiple_of(base + turn * LO, 128), LO)
        sub = sorted_ref[channels : channels + 1, at].astype(jnp.int32) - block * step
        lane = sorted_ref[channels + 1 : channels + 2, at].astype(jnp.int32)
        mask = to_f32(iota((step, LO), 0) == sub)
        mean = sorted_ref[:channels, at]
        tall = (mean[:, None, :] * mask[None]).reshape(channels * step, LO).astype(jnp.bfloat16)
        lane_hot = to_f32(iota((wide, LO), 0) == lane).astype(jnp.bfloat16)
        return lax.dot_general(tall, lane_hot, NT, preferred_element_type=jnp.float32)

    def put(value):
        out_ref[...] = value.astype(jnp.bfloat16).reshape(channels, step, wide)[:, :, :lanes]

    @pl.when(turns <= 1)
    def _():
        put(partial(0))

    @pl.when(turns > 1)
    def _():
        acc_ref[...] = partial(0)

        @pl.loop(1, turns)
        def _(turn):
            acc_ref[...] += partial(turn)

        put(acc_ref[...])


def place(sorted_values, starts, channels, subs, lanes):
    wide = round_up(lanes, 128)
    blocks = pl.cdiv(subs, STEP)
    return pl.pallas_call(
        lambda *refs: place_body(0, *refs),
        grid_spec=pltpu.PrefetchScalarGridSpec(
            num_scalar_prefetch=1,
            grid=(blocks,),
            in_specs=[pl.BlockSpec(sorted_values.shape, lambda b, s: (0, 0))],
            out_specs=pl.BlockSpec((channels, STEP, lanes), lambda b, s: (0, b, 0)),
            scratch_shapes=[pltpu.VMEM((channels * STEP, wide), jnp.float32)],
        ),
        out_shape=jax.ShapeDtypeStruct((channels, subs, lanes), jnp.bfloat16),
        compiler_params=pltpu.CompilerParams(dimension_semantics=("arbitrary",)),
        name="place",
    )(starts, sorted_values)


def on_device(
    point_feats,
    point_class,
    point_band,
    point_pillar,
    point_counts,
    pillar_cell,
    class_scores,
    encoder_weight,
    encoder_bias,
):
    band_count = lax.axis_size("bev")
    frames = lax.axis_size("pts")
    total = point_class.shape[0]
    pillars = pillar_cell.shape[-1]
    channels = encoder_weight.shape[0]
    band_rows = ROWS // band_count
    own = (
        point_feats,
        point_class.reshape(1, -1),
        point_band.reshape(1, -1),
        point_pillar.reshape(1, -1),
    )
    if band_count == 2:
        peer = tuple(lax.ppermute(x, "bev", [(0, 1), (1, 0)]) for x in own)
        points = own + peer
        spans = (lambda band: band, lambda band: 1 - band)
    else:
        gathered = [lax.all_gather(x, "bev", axis=0) for x in own]
        points = tuple(x[i] for i in range(band_count) for x in gathered)
        spans = tuple((lambda band, i=i: i) for i in range(band_count))
    parts = len(spans)

    def tiles(subs, lanes):
        return round_up(subs, 16) * round_up(lanes, 128)

    sub_of = "col" if tiles(COLS, band_rows) <= tiles(band_rows, COLS) else "row"
    subs, lanes = (COLS, band_rows) if sub_of == "col" else (band_rows, COLS)
    width = round_up(pillars, LO)
    vmem = pl.BlockSpec(memory_space=pltpu.VMEM)
    smem = pl.BlockSpec(memory_space=pltpu.SMEM)
    sorted_values, starts, tally = pl.pallas_call(
        lambda *refs: pool_body(parts, spans, pillars, sub_of, *refs),
        in_specs=[vmem] * (4 * parts) + [smem] + [vmem] * 4,
        out_specs=(vmem, vmem, vmem),
        out_shape=(
            jax.ShapeDtypeStruct((channels + 8, width + LO), jnp.float32),
            jax.ShapeDtypeStruct((1, 128), jnp.int32),
            jax.ShapeDtypeStruct((1, 128), jnp.float32),
        ),
        scratch_shapes=[pltpu.VMEM((1, width), jnp.int32)],
        name="pool",
    )(
        *points,
        point_counts,
        pillar_cell.reshape(1, pillars),
        class_scores,
        encoder_weight,
        encoder_bias.reshape(1, channels),
    )
    stride = 1
    while stride < frames:
        pairs = [(i, i ^ stride) for i in range(frames)]
        tally = tally + lax.ppermute(tally, "pts", pairs)
        stride *= 2
    class_counts = tally[0, :CLASSES] / total
    planes = place(sorted_values, starts, channels, subs, lanes)
    bev_image = planes.swapaxes(1, 2) if sub_of == "col" else planes
    return (bev_image[None], class_counts)


def solution(mesh):
    return jax.shard_map(
        on_device,
        mesh=mesh,
        in_specs=(
            P(None, ("pts", "bev")),
            P(("pts", "bev")),
            P(("pts", "bev")),
            P(("pts", "bev")),
            P(),
            P("pts", "bev", None),
            P(),
            P(),
            P(),
        ),
        out_specs=(P("pts", None, "bev", None), P()),
        check_vma=False,
    )
```

```python
import jax
import jax.numpy as jnp
from jax import lax
from jax.experimental import pallas as pl
from jax.experimental.pallas import tpu as pltpu
from jax.sharding import PartitionSpec as P

ROWS = 496
COLS = 432
CLASSES = 11

LO = 256
STEP = 16
BUCKETS = 32
GROUP = 3
LEADER_ONLY = False
HIGHEST = lax.Precision.HIGHEST
NT = (((1,), (1,)), ((), ()))


def round_up(value, unit):
    return -(-value // unit) * unit


def iota(shape, axis):
    return lax.broadcasted_iota(jnp.int32, shape, axis)


def to_f32(mask):
    return jnp.where(mask, 1.0, 0.0).astype(jnp.float32)


def split3(value):
    high = value.astype(jnp.bfloat16).astype(jnp.float32)
    rest = value - high
    mid = rest.astype(jnp.bfloat16).astype(jnp.float32)
    return high, mid, rest - mid


def encoder_matrix(weight_t, scores, bias_row):
    columns, channels = weight_t.shape
    lane = iota((columns, 80), 1)
    row = iota((columns, 80), 0)
    pick = to_f32((lane < 24) & ((lane & 3) == row))
    shift = to_f32(iota((columns, CLASSES), 0) == iota((columns, CLASSES), 1) + 4)
    place_lane = iota((CLASSES, 80), 1)
    place = to_f32((place_lane >= 32) & ((place_lane & 15) == iota((CLASSES, 80), 0)))
    spread = jnp.dot(
        jnp.dot(shift, scores, precision=HIGHEST, preferred_element_type=jnp.float32),
        place,
        precision=HIGHEST,
        preferred_element_type=jnp.float32,
    )
    matrix = lax.dot_general(
        weight_t,
        pick + spread,
        (((0,), (0,)), ((), ())),
        precision=HIGHEST,
        preferred_element_type=jnp.float32,
    )
    eye = iota((channels, channels), 0) == iota((channels, channels), 1)
    bias = jnp.sum(jnp.where(eye, bias_row, 0.0), axis=1, keepdims=True)
    out_lane = iota((channels, 80), 1)
    matrix = matrix + jnp.where((out_lane >= 32) & ((out_lane & 15) == CLASSES), bias, 0.0)
    high, mid, low = split3(matrix)
    take_mid = ((out_lane >= 8) & (out_lane < 16)) | ((out_lane >= 48) & (out_lane < 64))
    take_low = ((out_lane >= 16) & (out_lane < 20)) | (out_lane >= 64)
    return jnp.where(take_mid, mid, jnp.where(take_low, low, high)).astype(jnp.bfloat16)


def two_level(values, hi, lo, hi_count):
    _, total = values.shape
    tall = [values * to_f32(hi == h).astype(jnp.bfloat16) for h in range(hi_count)]
    one_hot = to_f32(iota((LO, total), 0) == lo).astype(jnp.bfloat16)
    return tall, one_hot


def tally_body(live_of, counts_ref, class_ref, tally_ref):
    classes = class_ref[...]
    live = live_of(counts_ref, classes.shape[1])
    total = classes.shape[1]
    one_hot = to_f32((iota((16, total), 0) == classes) & live)
    tally = jnp.sum(one_hot, axis=1, keepdims=True)
    diagonal = iota((16, 128), 0) == iota((16, 128), 1)
    tally_ref[...] = jnp.sum(jnp.where(diagonal, tally, 0.0), axis=0, keepdims=True)


def live_points(span, counts_ref, total):
    live_total = counts_ref[lax.axis_index("pts")]
    return span(lax.axis_index("bev")) * total + iota((1, total), 1) < live_total


def pool_part(span, hi_count, matrix, counts_ref, feats_ref, class_ref, band_ref, pillar_ref):
    feats = feats_ref[...]
    total = feats.shape[1]
    live = live_points(span, counts_ref, total)
    one_hot = to_f32(iota((16, total), 0) == class_ref[...])
    one_hot = jnp.where(iota((16, total), 0) == CLASSES, 1.0, one_hot)
    high, mid, low = split3(jnp.concatenate([feats, feats], axis=0))
    top = iota((8, total), 0) < 4
    first = jnp.where(top, high, mid)
    third = jnp.where(top, high, low)
    stacked = jnp.concatenate(
        [first, first, third, jnp.zeros_like(first), one_hot, one_hot, one_hot], axis=0
    ).astype(jnp.bfloat16)
    hidden = jnp.dot(matrix, stacked, preferred_element_type=jnp.float32)
    encoded = jnp.maximum(hidden, 0.0).astype(jnp.bfloat16)
    pillar = pillar_ref[...]
    hi = jnp.where(live & (band_ref[...] == lax.axis_index("bev")), pillar >> 8, 15)
    lo = pillar & (LO - 1)
    tall, lo_hot = two_level(encoded, hi, lo, hi_count)
    tall.append(to_f32(iota((16, total), 0) == hi).astype(jnp.bfloat16))
    return lax.dot_general(
        jnp.concatenate(tall, axis=0), lo_hot, NT, preferred_element_type=jnp.float32
    )


def first_body(span, pillars, counts_ref, scores_ref, weight_ref, bias_ref, *refs):
    hi_count = round_up(pillars, LO) // LO
    sums_ref, matrix_ref = refs[4:]
    matrix = encoder_matrix(weight_ref[...], scores_ref[...], bias_ref[...])
    matrix_ref[...] = matrix
    sums_ref[...] = pool_part(span, hi_count, matrix, counts_ref, *refs[:4])


def second_body(spans, pillars, sub_of, counts_ref, matrix_ref, sums_in_ref, cell_ref, *refs):
    parts = len(spans)
    sorted_ref, starts_ref, cell_pad = refs[4 * parts :]
    channels = matrix_ref.shape[0]
    hi_count = round_up(pillars, LO) // LO
    width = hi_count * LO
    sums = sums_in_ref[...]
    for part in range(parts):
        sums = sums + pool_part(
            spans[part], hi_count, matrix_ref[...], counts_ref, *refs[4 * part : 4 * part + 4]
        )

    cell_pad[...] = jnp.full(cell_pad.shape, -1, jnp.int32)
    cell_pad[:, :pillars] = cell_ref[...].reshape(1, pillars)
    cell = cell_pad[...]
    cell_f = cell.astype(jnp.float32)
    grid_row = jnp.floor((cell_f + 0.5) * (1.0 / COLS)).astype(jnp.int32)
    grid_col = cell - grid_row * COLS
    sub, lane = (grid_col, grid_row) if sub_of == "col" else (grid_row, grid_col)
    block = jnp.where(cell >= 0, sub >> 4, BUCKETS - 1)
    member = to_f32(iota((BUCKETS, width), 0) == block)
    before = to_f32(iota((LO, LO), 0) < iota((LO, LO), 1)).astype(jnp.bfloat16)
    offset = jnp.zeros((BUCKETS, 1), jnp.float32)
    ranks = []
    for h in range(hi_count):
        chunk = member[:, h * LO : (h + 1) * LO]
        prefix = jnp.dot(
            chunk.astype(jnp.bfloat16), before, preferred_element_type=jnp.float32
        )
        ranks.append(prefix + offset)
        offset = offset + jnp.sum(chunk, axis=1, keepdims=True)
    square = iota((BUCKETS, 128), 0)
    across = iota((BUCKETS, 128), 1)
    starts_row = jnp.sum(jnp.where(square < across, offset, 0.0), axis=0, keepdims=True)
    size_row = jnp.sum(jnp.where(square == across, offset, 0.0), axis=0, keepdims=True)
    starts_i = starts_row.astype(jnp.int32)
    reach = (starts_i & 127) + size_row.astype(jnp.int32)
    real = iota((1, 128), 1) < BUCKETS - 1
    wide = jnp.max(jnp.where(real, reach, 0), axis=1, keepdims=True) > LO
    starts_ref[...] = jnp.where(iota((1, 128), 1) == 127, wide.astype(jnp.int32), starts_i)
    start = jnp.sum(jnp.where(square == across, starts_row, 0.0), axis=1, keepdims=True)
    placed = jnp.zeros((hi_count * (channels + 16), LO), jnp.float32)
    extra = iota((16, LO), 0)
    counts = sums[hi_count * channels :]
    for h in range(hi_count):
        at = slice(h * LO, (h + 1) * LO)
        rank = jnp.sum(member[:, at] * (ranks[h] + start), axis=0, keepdims=True).astype(jnp.int32)
        mean = sums[h * channels : (h + 1) * channels] / jnp.maximum(counts[h : h + 1], 1.0)
        sub_h = sub[:, at]
        lane_h = lane[:, at]
        where = jnp.where(
            extra == 0,
            block[:, at],
            jnp.where(
                extra == 1,
                sub_h & (STEP - 1),
                jnp.where(extra == 2, lane_h >> 8, jnp.where(extra == 3, lane_h & 255, 0)),
            ),
        ).astype(jnp.float32)
        values = jnp.concatenate([mean, where], axis=0).astype(jnp.bfloat16)
        tall, lo_hot = two_level(values, rank >> 8, rank & (LO - 1), hi_count)
        placed = placed + lax.dot_general(
            jnp.concatenate(tall, axis=0), lo_hot, NT, preferred_element_type=jnp.float32
        )
    rows = channels + 16
    tail = iota((8, LO), 0)
    for h in range(hi_count):
        piece = placed[h * rows : (h + 1) * rows]
        sub_s = piece[channels : channels + 1] * STEP + piece[channels + 1 : channels + 2]
        lane_s = piece[channels + 2 : channels + 3] * 256.0 + piece[channels + 3 : channels + 4]
        extra_s = jnp.where(tail == 0, sub_s, jnp.where(tail == 1, lane_s, 0.0))
        for half in range(2):
            at = slice(half * 128, half * 128 + 128)
            sorted_ref[2 * h + half, :channels, :] = piece[:channels, at]
            sorted_ref[2 * h + half, channels:, :] = extra_s[:, at]
    for chunk in range(2 * hi_count, 2 * hi_count + 2):
        sorted_ref[chunk, :channels, :] = jnp.zeros((channels, 128), jnp.float32)
        sorted_ref[chunk, channels:, :] = jnp.full((8, 128), -1.0, jnp.float32)


def place_body(starts_ref, sorted_ref, out_ref, image, lane_hot, acc_ref, sems):
    channels, _, lanes = out_ref.shape
    chunks, wide, _ = lane_hot.shape
    blocks = image.shape[1] // STEP
    for chunk in range(chunks):
        lane = sorted_ref[chunk, channels + 1 : channels + 2, :].astype(jnp.int32)
        lane_hot[chunk] = to_f32(iota((wide, 128), 0) == lane).astype(jnp.bfloat16)

    def base_of(block):
        return starts_ref[0, block] >> 7

    def partial(block, turn):
        talls = []
        hots = []
        for half in range(2):
            chunk = base_of(block) + 2 * turn + half
            sub = sorted_ref[chunk, channels : channels + 1, :].astype(jnp.int32) - block * STEP
            mask_a = to_f32(iota((8, 128), 0) == sub)
            mask_b = to_f32(iota((8, 128), 0) + 8 == sub)
            tall = []
            for channel in range(channels):
                row = sorted_ref[chunk, pl.ds(channel, 8, stride=0), :]
                tall.append(
                    jnp.concatenate([row * mask_a, row * mask_b], axis=0).astype(jnp.bfloat16)
                )
            talls.append(jnp.concatenate(tall, axis=0))
            hots.append(lane_hot[chunk])
        return lax.dot_general(
            jnp.concatenate(talls, axis=1),
            jnp.concatenate(hots, axis=1),
            NT,
            preferred_element_type=jnp.float32,
        )

    def put(block, value):
        rows = pl.ds(block * STEP, STEP)
        tile = value.astype(jnp.bfloat16).reshape(channels, STEP, wide)
        image[:, rows, :] = tile[:, :, :lanes]

    spans = []
    for begin in range(0, blocks, GROUP):
        spans.append((begin, min(begin + GROUP, blocks)))
    copies = []
    for index, (begin, end) in enumerate(spans):
        rows = pl.ds(begin * STEP, (end - begin) * STEP)
        copies.append(
            pltpu.make_async_copy(image.at[:, rows], out_ref.at[:, rows], sems.at[index])
        )
    spread = starts_ref[0, 127]

    @pl.when(spread == 0)
    def _():
        for (begin, end), copy in zip(spans, copies):
            for block in range(begin, end):
                put(block, partial(block, 0))
            copy.start()

    @pl.when(spread != 0)
    def _():
        @pl.loop(0, blocks)
        def _(block):
            turns = (starts_ref[0, block + 1] - base_of(block) * 128 + LO - 1) // LO
            acc_ref[...] = partial(block, 0)

            @pl.loop(1, turns)
            def _(turn):
                acc_ref[...] += partial(block, turn)

            put(pl.multiple_of(block, 1), acc_ref[...])

        for copy in copies:
            copy.start()

    for copy in copies:
        copy.wait()


def place(sorted_values, starts, channels, subs, lanes):
    wide = round_up(lanes, 128)
    blocks = pl.cdiv(subs, STEP)
    groups = pl.cdiv(blocks, GROUP)
    return pl.pallas_call(
        place_body,
        in_specs=[
            pl.BlockSpec(memory_space=pltpu.SMEM),
            pl.BlockSpec(memory_space=pltpu.VMEM),
        ],
        out_specs=pl.BlockSpec(memory_space=pl.ANY),
        scratch_shapes=[
            pltpu.VMEM((channels, blocks * STEP, lanes), jnp.bfloat16),
            pltpu.VMEM((sorted_values.shape[0], wide, 128), jnp.bfloat16),
            pltpu.VMEM((channels * STEP, wide), jnp.float32),
            pltpu.SemaphoreType.DMA((groups,)),
        ],
        out_shape=jax.ShapeDtypeStruct((channels, blocks * STEP, lanes), jnp.bfloat16),
        cost_estimate=pl.CostEstimate(flops=10**9, transcendentals=0, bytes_accessed=10**7),
        name="place",
    )(starts, sorted_values)[:, :subs]


def all_tallies(tally, frames, band_count):
    both = ("pts", "bev")
    leader = band_count - 1
    total = tally
    for shift in range(1, band_count):
        pairs = [((i + shift) % band_count, i) for i in range(band_count)]
        total = total + lax.ppermute(tally, "bev", pairs)
    stride = 1
    while stride < frames:
        radix = 4 if frames % (stride * 4) == 0 else 2
        received = []
        for hop in range(1, radix):
            pairs = []
            for i in range(frames):
                j = i ^ (hop * stride)
                if LEADER_ONLY:
                    pairs.append((i * band_count + leader, j * band_count + leader))
                else:
                    pairs.extend((i * band_count + k, j * band_count + k) for k in range(band_count))
            received.append(lax.ppermute(total, both, pairs))
        total = total + sum(received)
        stride *= radix
    if LEADER_ONLY:
        given = [
            lax.ppermute(total, "bev", [(leader, k)])
            for k in range(band_count)
            if k != leader
        ]
        total = jnp.where(lax.axis_index("bev") == leader, total, sum(given))
    return total


def on_device(
    point_feats,
    point_class,
    point_band,
    point_pillar,
    point_counts,
    pillar_cell,
    class_scores,
    encoder_weight,
    encoder_bias,
):
    band_count = lax.axis_size("bev")
    frames = lax.axis_size("pts")
    total = point_class.shape[0]
    pillars = pillar_cell.shape[-1]
    channels = encoder_weight.shape[0]
    band_rows = ROWS // band_count
    own = (
        point_feats,
        point_class.reshape(1, -1),
        point_band.reshape(1, -1),
        point_pillar.reshape(1, -1),
    )
    others = []
    for shift in range(1, band_count):
        pairs = [((i + shift) % band_count, i) for i in range(band_count)]
        others.extend(lax.ppermute(x, "bev", pairs) for x in own)
    spans = [lambda band, k=k: (band + k) % band_count for k in range(1, band_count)]

    def own_span(band):
        return band

    def tiles(subs, lanes):
        return round_up(subs, 16) * round_up(lanes, 128)

    sub_of = "col" if tiles(COLS, band_rows) <= tiles(band_rows, COLS) else "row"
    subs, lanes = (COLS, band_rows) if sub_of == "col" else (band_rows, COLS)
    width = round_up(pillars, LO)
    vmem = pl.BlockSpec(memory_space=pltpu.VMEM)
    smem = pl.BlockSpec(memory_space=pltpu.SMEM)
    tally = pl.pallas_call(
        lambda *refs: tally_body(lambda c, t: live_points(own_span, c, t), *refs),
        in_specs=[smem, vmem],
        out_specs=vmem,
        out_shape=jax.ShapeDtypeStruct((1, 128), jnp.float32),
        name="tally",
    )(point_counts, own[1])
    class_counts = (all_tallies(tally, frames, band_count) / total)[0, :CLASSES]
    hi_count = width // LO
    sums, matrix = pl.pallas_call(
        lambda *refs: first_body(own_span, pillars, *refs),
        in_specs=[smem] + [vmem] * 7,
        out_specs=(vmem, vmem),
        out_shape=(
            jax.ShapeDtypeStruct((hi_count * channels + 16, LO), jnp.float32),
            jax.ShapeDtypeStruct((channels, 80), jnp.bfloat16),
        ),
        cost_estimate=pl.CostEstimate(flops=10**9, transcendentals=0, bytes_accessed=10**6),
        name="pool_own",
    )(
        point_counts,
        class_scores,
        encoder_weight.T,
        encoder_bias.reshape(1, channels),
        *own,
    )
    sorted_values, starts = pl.pallas_call(
        lambda *refs: second_body(spans, pillars, sub_of, *refs),
        in_specs=[smem] + [vmem] * (3 + len(others)),
        out_specs=(vmem, vmem),
        out_shape=(
            jax.ShapeDtypeStruct(((width + LO) // 128, channels + 8, 128), jnp.float32),
            jax.ShapeDtypeStruct((1, 128), jnp.int32),
        ),
        scratch_shapes=[pltpu.VMEM((1, width), jnp.int32)],
        cost_estimate=pl.CostEstimate(flops=10**9, transcendentals=0, bytes_accessed=10**6),
        name="pool_rest",
    )(point_counts, matrix, sums, pillar_cell.reshape(1, pillars), *others)
    planes = place(sorted_values, starts, channels, subs, lanes)
    bev_image = planes.swapaxes(1, 2) if sub_of == "col" else planes
    return (bev_image[None], class_counts)


def solution(mesh):
    return jax.shard_map(
        on_device,
        mesh=mesh,
        in_specs=(
            P(None, ("pts", "bev")),
            P(("pts", "bev")),
            P(("pts", "bev")),
            P(("pts", "bev")),
            P(),
            P("pts", "bev", None),
            P(),
            P(),
            P(),
        ),
        out_specs=(P("pts", None, "bev", None), P()),
        check_vma=False,
    )
```

```python
import jax
import jax.numpy as jnp
from jax import lax
from jax.experimental import pallas as pl
from jax.experimental.pallas import tpu as pltpu
from jax.sharding import PartitionSpec as P

ROWS = 496
COLS = 432
CLASSES = 11

LO = 256
STEP = 16
BUCKETS = 32
GROUP = 3
HIGHEST = lax.Precision.HIGHEST
NT = (((1,), (1,)), ((), ()))


def round_up(value, unit):
    return -(-value // unit) * unit


def iota(shape, axis):
    return lax.broadcasted_iota(jnp.int32, shape, axis)


def to_f32(mask):
    return jnp.where(mask, 1.0, 0.0).astype(jnp.float32)


def split3(value):
    high = value.astype(jnp.bfloat16).astype(jnp.float32)
    rest = value - high
    mid = rest.astype(jnp.bfloat16).astype(jnp.float32)
    return high, mid, rest - mid


def encoder_matrix(weight_t, scores, bias_row):
    columns, channels = weight_t.shape
    lane = iota((columns, 80), 1)
    row = iota((columns, 80), 0)
    pick = to_f32((lane < 24) & ((lane & 3) == row))
    shift = to_f32(iota((columns, CLASSES), 0) == iota((columns, CLASSES), 1) + 4)
    place_lane = iota((CLASSES, 80), 1)
    place = to_f32((place_lane >= 32) & ((place_lane & 15) == iota((CLASSES, 80), 0)))
    spread = jnp.dot(
        jnp.dot(shift, scores, precision=HIGHEST, preferred_element_type=jnp.float32),
        place,
        precision=HIGHEST,
        preferred_element_type=jnp.float32,
    )
    matrix = lax.dot_general(
        weight_t,
        pick + spread,
        (((0,), (0,)), ((), ())),
        precision=HIGHEST,
        preferred_element_type=jnp.float32,
    )
    eye = iota((channels, channels), 0) == iota((channels, channels), 1)
    bias = jnp.sum(jnp.where(eye, bias_row, 0.0), axis=1, keepdims=True)
    out_lane = iota((channels, 80), 1)
    matrix = matrix + jnp.where((out_lane >= 32) & ((out_lane & 15) == CLASSES), bias, 0.0)
    high, mid, low = split3(matrix)
    take_mid = ((out_lane >= 8) & (out_lane < 16)) | ((out_lane >= 48) & (out_lane < 64))
    take_low = ((out_lane >= 16) & (out_lane < 20)) | (out_lane >= 64)
    return jnp.where(take_mid, mid, jnp.where(take_low, low, high)).astype(jnp.bfloat16)


def two_level(values, hi, lo, hi_count):
    _, total = values.shape
    tall = [values * to_f32(hi == h).astype(jnp.bfloat16) for h in range(hi_count)]
    one_hot = to_f32(iota((LO, total), 0) == lo).astype(jnp.bfloat16)
    return tall, one_hot


def class_tally(spans, counts_ref, class_refs):
    tally = jnp.zeros((16, 128), jnp.float32)
    for span, class_ref in zip(spans, class_refs):
        classes = class_ref[...]
        total = classes.shape[1]
        live = live_points(span, counts_ref, total)
        one_hot = to_f32((iota((16, total), 0) == classes) & live)
        for begin in range(0, total, 128):
            tally = tally + one_hot[:, begin : begin + 128]
    tally = jnp.sum(tally, axis=1, keepdims=True)
    diagonal = iota((16, 128), 0) == iota((16, 128), 1)
    return jnp.sum(jnp.where(diagonal, tally, 0.0), axis=0, keepdims=True)


def live_points(span, counts_ref, total):
    live_total = counts_ref[lax.axis_index("pts")]
    return span(lax.axis_index("bev")) * total + iota((1, total), 1) < live_total


def pool_part(span, hi_count, matrix, counts_ref, feats_ref, class_ref, band_ref, pillar_ref):
    feats = feats_ref[...]
    total = feats.shape[1]
    live = live_points(span, counts_ref, total)
    one_hot = to_f32(iota((16, total), 0) == class_ref[...])
    one_hot = jnp.where(iota((16, total), 0) == CLASSES, 1.0, one_hot)
    high, mid, low = split3(jnp.concatenate([feats, feats], axis=0))
    top = iota((8, total), 0) < 4
    first = jnp.where(top, high, mid)
    third = jnp.where(top, high, low)
    stacked = jnp.concatenate(
        [first, first, third, jnp.zeros_like(first), one_hot, one_hot, one_hot], axis=0
    ).astype(jnp.bfloat16)
    hidden = jnp.dot(matrix, stacked, preferred_element_type=jnp.float32)
    encoded = jnp.maximum(hidden, 0.0).astype(jnp.bfloat16)
    pillar = pillar_ref[...]
    hi = jnp.where(live & (band_ref[...] == lax.axis_index("bev")), pillar >> 8, 15)
    lo = pillar & (LO - 1)
    tall, lo_hot = two_level(encoded, hi, lo, hi_count)
    tall.append(to_f32(iota((16, total), 0) == hi).astype(jnp.bfloat16))
    return lax.dot_general(
        jnp.concatenate(tall, axis=0), lo_hot, NT, preferred_element_type=jnp.float32
    )


def first_body(span, spans, pillars, counts_ref, scores_ref, weight_ref, bias_ref, *refs):
    hi_count = round_up(pillars, LO) // LO
    own, other_classes = refs[:4], refs[4 : 4 + len(spans)]
    sums_ref, matrix_ref, tally_ref = refs[4 + len(spans) :]
    tally_ref[...] = class_tally([span, *spans], counts_ref, [own[1], *other_classes])
    matrix = encoder_matrix(weight_ref[...], scores_ref[...], bias_ref[...])
    matrix_ref[...] = matrix
    sums_ref[...] = pool_part(span, hi_count, matrix, counts_ref, *own)


def second_body(spans, pillars, sub_of, counts_ref, matrix_ref, sums_in_ref, cell_ref, *refs):
    parts = len(spans)
    sorted_ref, starts_ref, cell_pad = refs[4 * parts :]
    channels = matrix_ref.shape[0]
    hi_count = round_up(pillars, LO) // LO
    width = hi_count * LO
    sums = sums_in_ref[...]
    for part in range(parts):
        sums = sums + pool_part(
            spans[part], hi_count, matrix_ref[...], counts_ref, *refs[4 * part : 4 * part + 4]
        )

    cell_pad[...] = jnp.full(cell_pad.shape, -1, jnp.int32)
    cell_pad[:, :pillars] = cell_ref[...].reshape(1, pillars)
    cell = cell_pad[...]
    cell_f = cell.astype(jnp.float32)
    grid_row = jnp.floor((cell_f + 0.5) * (1.0 / COLS)).astype(jnp.int32)
    grid_col = cell - grid_row * COLS
    sub, lane = (grid_col, grid_row) if sub_of == "col" else (grid_row, grid_col)
    block = jnp.where(cell >= 0, sub >> 4, BUCKETS - 1)
    member = to_f32(iota((BUCKETS, width), 0) == block)
    before = to_f32(iota((LO, LO), 0) < iota((LO, LO), 1)).astype(jnp.bfloat16)
    offset = jnp.zeros((BUCKETS, 1), jnp.float32)
    ranks = []
    for h in range(hi_count):
        chunk = member[:, h * LO : (h + 1) * LO]
        prefix = jnp.dot(
            chunk.astype(jnp.bfloat16), before, preferred_element_type=jnp.float32
        )
        ranks.append(prefix + offset)
        offset = offset + jnp.sum(chunk, axis=1, keepdims=True)
    square = iota((BUCKETS, 128), 0)
    across = iota((BUCKETS, 128), 1)
    starts_row = jnp.sum(jnp.where(square < across, offset, 0.0), axis=0, keepdims=True)
    size_row = jnp.sum(jnp.where(square == across, offset, 0.0), axis=0, keepdims=True)
    starts_i = starts_row.astype(jnp.int32)
    reach = (starts_i & 127) + size_row.astype(jnp.int32)
    real = iota((1, 128), 1) < BUCKETS - 1
    wide = jnp.max(jnp.where(real, reach, 0), axis=1, keepdims=True) > LO
    starts_ref[...] = jnp.where(iota((1, 128), 1) == 127, wide.astype(jnp.int32), starts_i)
    start = jnp.sum(jnp.where(square == across, starts_row, 0.0), axis=1, keepdims=True)
    placed = jnp.zeros((hi_count * (channels + 16), LO), jnp.float32)
    extra = iota((16, LO), 0)
    counts = sums[hi_count * channels :]
    for h in range(hi_count):
        at = slice(h * LO, (h + 1) * LO)
        rank = jnp.sum(member[:, at] * (ranks[h] + start), axis=0, keepdims=True).astype(jnp.int32)
        mean = sums[h * channels : (h + 1) * channels] / jnp.maximum(counts[h : h + 1], 1.0)
        sub_h = sub[:, at]
        lane_h = lane[:, at]
        where = jnp.where(
            extra == 0,
            block[:, at],
            jnp.where(
                extra == 1,
                sub_h & (STEP - 1),
                jnp.where(extra == 2, lane_h >> 8, jnp.where(extra == 3, lane_h & 255, 0)),
            ),
        ).astype(jnp.float32)
        values = jnp.concatenate([mean, where], axis=0).astype(jnp.bfloat16)
        tall, lo_hot = two_level(values, rank >> 8, rank & (LO - 1), hi_count)
        placed = placed + lax.dot_general(
            jnp.concatenate(tall, axis=0), lo_hot, NT, preferred_element_type=jnp.float32
        )
    rows = channels + 16
    tail = iota((8, LO), 0)
    for h in range(hi_count):
        piece = placed[h * rows : (h + 1) * rows]
        sub_s = piece[channels : channels + 1] * STEP + piece[channels + 1 : channels + 2]
        lane_s = piece[channels + 2 : channels + 3] * 256.0 + piece[channels + 3 : channels + 4]
        extra_s = jnp.where(tail == 0, sub_s, jnp.where(tail == 1, lane_s, 0.0))
        for half in range(2):
            at = slice(half * 128, half * 128 + 128)
            sorted_ref[2 * h + half, :channels, :] = piece[:channels, at]
            sorted_ref[2 * h + half, channels:, :] = extra_s[:, at]
    for chunk in range(2 * hi_count, 2 * hi_count + 2):
        sorted_ref[chunk, :channels, :] = jnp.zeros((channels, 128), jnp.float32)
        sorted_ref[chunk, channels:, :] = jnp.full((8, 128), -1.0, jnp.float32)


def place_body(starts_vmem, sorted_ref, out_ref, starts_ref, image, lane_hot, acc_ref, sem, sems):
    fetch = pltpu.make_async_copy(starts_vmem, starts_ref, sem)
    fetch.start()
    fetch.wait()
    channels, _, lanes = out_ref.shape
    chunks, wide, _ = lane_hot.shape
    blocks = image.shape[1] // STEP

    def hot_of(chunk):
        lane = sorted_ref[chunk, channels + 1 : channels + 2, :].astype(jnp.int32)
        return to_f32(iota((wide, 128), 0) == lane).astype(jnp.bfloat16)

    def base_of(block):
        return starts_ref[0, block] >> 7

    def partial(block, turn, ready=True):
        talls = []
        hots = []
        for half in range(2):
            chunk = base_of(block) + 2 * turn + half
            sub = sorted_ref[chunk, channels : channels + 1, :].astype(jnp.int32) - block * STEP
            mask_a = to_f32(iota((8, 128), 0) == sub)
            mask_b = to_f32(iota((8, 128), 0) + 8 == sub)
            tall = []
            for channel in range(channels):
                row = sorted_ref[chunk, pl.ds(channel, 8, stride=0), :]
                tall.append(
                    jnp.concatenate([row * mask_a, row * mask_b], axis=0).astype(jnp.bfloat16)
                )
            talls.append(jnp.concatenate(tall, axis=0))
            hots.append(lane_hot[chunk] if ready else hot_of(chunk))
        return lax.dot_general(
            jnp.concatenate(talls, axis=1),
            jnp.concatenate(hots, axis=1),
            NT,
            preferred_element_type=jnp.float32,
        )

    def put(block, value):
        rows = pl.ds(block * STEP, STEP)
        tile = value.astype(jnp.bfloat16).reshape(channels, STEP, wide)
        image[:, rows, :] = tile[:, :, :lanes]

    spans = []
    begin = 0
    while begin < blocks:
        end = min(begin + min(len(spans) + 1, GROUP), blocks)
        spans.append((begin, end))
        begin = end
    copies = []
    for index, (begin, end) in enumerate(spans):
        rows = pl.ds(begin * STEP, (end - begin) * STEP)
        copies.append(
            pltpu.make_async_copy(image.at[:, rows], out_ref.at[:, rows], sems.at[index])
        )
    spread = starts_ref[0, 127]

    @pl.when(spread == 0)
    def _():
        put(0, partial(0, 0, ready=False))
        copies[0].start()
        for chunk in range(chunks):
            lane_hot[chunk] = hot_of(chunk)
        for (begin, end), copy in zip(spans[1:], copies[1:]):
            for block in range(begin, end):
                put(block, partial(block, 0))
            copy.start()

    @pl.when(spread != 0)
    def _():
        @pl.loop(0, blocks)
        def _(block):
            turns = (starts_ref[0, block + 1] - base_of(block) * 128 + LO - 1) // LO
            acc_ref[...] = partial(block, 0, ready=False)

            @pl.loop(1, turns)
            def _(turn):
                acc_ref[...] += partial(block, turn, ready=False)

            put(pl.multiple_of(block, 1), acc_ref[...])

        for copy in copies:
            copy.start()

    for copy in copies:
        copy.wait()


def place(sorted_values, starts, channels, subs, lanes):
    wide = round_up(lanes, 128)
    blocks = pl.cdiv(subs, STEP)
    return pl.pallas_call(
        place_body,
        in_specs=[
            pl.BlockSpec(memory_space=pltpu.VMEM),
            pl.BlockSpec(memory_space=pltpu.VMEM),
        ],
        out_specs=pl.BlockSpec(memory_space=pl.ANY),
        scratch_shapes=[
            pltpu.SMEM((1, 128), jnp.int32),
            pltpu.VMEM((channels, blocks * STEP, lanes), jnp.bfloat16),
            pltpu.VMEM((sorted_values.shape[0], wide, 128), jnp.bfloat16),
            pltpu.VMEM((channels * STEP, wide), jnp.float32),
            pltpu.SemaphoreType.DMA,
            pltpu.SemaphoreType.DMA((blocks,)),
        ],
        out_shape=jax.ShapeDtypeStruct((channels, blocks * STEP, lanes), jnp.bfloat16),
        cost_estimate=pl.CostEstimate(flops=10**9, transcendentals=0, bytes_accessed=10**7),
        name="place",
    )(in_vmem(starts), in_vmem(sorted_values))[:, :subs]


def in_vmem(value):
    return pltpu.with_memory_space_constraint(value, pltpu.VMEM)


def all_tallies(total, frames):
    stride = 1
    while stride < frames:
        radix = 4 if frames % (stride * 4) == 0 else 2
        received = []
        for hop in range(1, radix):
            pairs = [(i, i ^ (hop * stride)) for i in range(frames)]
            received.append(lax.ppermute(total, "pts", pairs))
        total = total + sum(received)
        stride *= radix
    return total


def on_device(
    point_feats,
    point_class,
    point_band,
    point_pillar,
    point_counts,
    pillar_cell,
    class_scores,
    encoder_weight,
    encoder_bias,
):
    band_count = lax.axis_size("bev")
    frames = lax.axis_size("pts")
    total = point_class.shape[0]
    pillars = pillar_cell.shape[-1]
    channels = encoder_weight.shape[0]
    band_rows = ROWS // band_count
    own = (
        point_feats,
        point_class.reshape(1, -1),
        point_band.reshape(1, -1),
        point_pillar.reshape(1, -1),
    )
    shifts = [
        [((i + shift) % band_count, i) for i in range(band_count)]
        for shift in range(1, band_count)
    ]
    other_classes = [in_vmem(lax.ppermute(own[1], "bev", pairs)) for pairs in shifts]
    others = []
    for pairs, classes in zip(shifts, other_classes):
        band, pillar, feats = [
            in_vmem(lax.ppermute(own[index], "bev", pairs)) for index in (2, 3, 0)
        ]
        others.extend((feats, classes, band, pillar))
    spans = [lambda band, k=k: (band + k) % band_count for k in range(1, band_count)]

    def own_span(band):
        return band

    def tiles(subs, lanes):
        return round_up(subs, 16) * round_up(lanes, 128)

    sub_of = "col" if tiles(COLS, band_rows) <= tiles(band_rows, COLS) else "row"
    subs, lanes = (COLS, band_rows) if sub_of == "col" else (band_rows, COLS)
    width = round_up(pillars, LO)
    vmem = pl.BlockSpec(memory_space=pltpu.VMEM)
    smem = pl.BlockSpec(memory_space=pltpu.SMEM)
    hi_count = width // LO
    sums, matrix, tally = pl.pallas_call(
        lambda *refs: first_body(own_span, spans, pillars, *refs),
        in_specs=[smem] + [vmem] * (7 + len(other_classes)),
        out_specs=(vmem, vmem, vmem),
        out_shape=(
            pltpu.VMEM((hi_count * channels + 16, LO), jnp.float32),
            pltpu.VMEM((channels, 80), jnp.bfloat16),
            pltpu.VMEM((1, 128), jnp.float32),
        ),
        cost_estimate=pl.CostEstimate(flops=10**9, transcendentals=0, bytes_accessed=10**6),
        name="pool_own",
    )(
        point_counts,
        class_scores,
        encoder_weight.T,
        encoder_bias.reshape(1, channels),
        *own,
        *other_classes,
    )
    class_counts = (all_tallies(tally, frames) / total)[0, :CLASSES]
    sorted_values, starts = pl.pallas_call(
        lambda *refs: second_body(spans, pillars, sub_of, *refs),
        in_specs=[smem] + [vmem] * (3 + len(others)),
        out_specs=(vmem, vmem),
        out_shape=(
            pltpu.VMEM(((width + LO) // 128, channels + 8, 128), jnp.float32),
            pltpu.VMEM((1, 128), jnp.int32),
        ),
        scratch_shapes=[pltpu.VMEM((1, width), jnp.int32)],
        cost_estimate=pl.CostEstimate(flops=10**9, transcendentals=0, bytes_accessed=10**6),
        name="pool_rest",
    )(
        point_counts,
        in_vmem(matrix),
        in_vmem(sums),
        pillar_cell.reshape(1, pillars),
        *others,
    )
    planes = place(sorted_values, starts, channels, subs, lanes)
    bev_image = planes.swapaxes(1, 2) if sub_of == "col" else planes
    return (bev_image[None], class_counts)


def solution(mesh):
    return jax.shard_map(
        on_device,
        mesh=mesh,
        in_specs=(
            P(None, ("pts", "bev")),
            P(("pts", "bev")),
            P(("pts", "bev")),
            P(("pts", "bev")),
            P(),
            P("pts", "bev", None),
            P(),
            P(),
            P(),
        ),
        out_specs=(P("pts", None, "bev", None), P()),
        check_vma=False,
    )
```

```python
import jax
import jax.numpy as jnp
from jax import lax
from jax.experimental import pallas as pl
from jax.experimental.pallas import tpu as pltpu
from jax.sharding import PartitionSpec as P

ROWS = 496
COLS = 432
CLASSES = 11

LO = 256
STEP = 16
BUCKETS = 32
GROUP = 3
HIGHEST = lax.Precision.HIGHEST
NT = (((1,), (1,)), ((), ()))


def round_up(value, unit):
    return -(-value // unit) * unit


def iota(shape, axis):
    return lax.broadcasted_iota(jnp.int32, shape, axis)


def to_f32(mask):
    return jnp.where(mask, 1.0, 0.0).astype(jnp.float32)


def split3(value):
    high = value.astype(jnp.bfloat16).astype(jnp.float32)
    rest = value - high
    mid = rest.astype(jnp.bfloat16).astype(jnp.float32)
    return high, mid, rest - mid


def encoder_matrix(weight_t, scores, bias_row):
    columns, channels = weight_t.shape
    lane = iota((columns, 80), 1)
    row = iota((columns, 80), 0)
    pick = to_f32((lane < 24) & ((lane & 3) == row))
    shift = to_f32(iota((columns, CLASSES), 0) == iota((columns, CLASSES), 1) + 4)
    place_lane = iota((CLASSES, 80), 1)
    place = to_f32((place_lane >= 32) & ((place_lane & 15) == iota((CLASSES, 80), 0)))
    spread = jnp.dot(
        jnp.dot(shift, scores, precision=HIGHEST, preferred_element_type=jnp.float32),
        place,
        precision=HIGHEST,
        preferred_element_type=jnp.float32,
    )
    matrix = lax.dot_general(
        weight_t,
        pick + spread,
        (((0,), (0,)), ((), ())),
        precision=HIGHEST,
        preferred_element_type=jnp.float32,
    )
    eye = iota((channels, channels), 0) == iota((channels, channels), 1)
    bias = jnp.sum(jnp.where(eye, bias_row, 0.0), axis=1, keepdims=True)
    out_lane = iota((channels, 80), 1)
    matrix = matrix + jnp.where((out_lane >= 32) & ((out_lane & 15) == CLASSES), bias, 0.0)
    high, mid, low = split3(matrix)
    take_mid = ((out_lane >= 8) & (out_lane < 16)) | ((out_lane >= 48) & (out_lane < 64))
    take_low = ((out_lane >= 16) & (out_lane < 20)) | (out_lane >= 64)
    return jnp.where(take_mid, mid, jnp.where(take_low, low, high)).astype(jnp.bfloat16)


def two_level(values, hi, lo, hi_count):
    _, total = values.shape
    tall = [values * to_f32(hi == h).astype(jnp.bfloat16) for h in range(hi_count)]
    one_hot = to_f32(iota((LO, total), 0) == lo).astype(jnp.bfloat16)
    return tall, one_hot


def class_tally(spans, counts_ref, class_refs):
    tally = jnp.zeros((16, 128), jnp.float32)
    for span, class_ref in zip(spans, class_refs):
        classes = class_ref[...]
        total = classes.shape[1]
        live = live_points(span, counts_ref, total)
        one_hot = to_f32((iota((16, total), 0) == classes) & live)
        for begin in range(0, total, 128):
            tally = tally + one_hot[:, begin : begin + 128]
    tally = jnp.sum(tally, axis=1, keepdims=True)
    diagonal = iota((16, 128), 0) == iota((16, 128), 1)
    return jnp.sum(jnp.where(diagonal, tally, 0.0), axis=0, keepdims=True)


def live_points(span, counts_ref, total):
    counts = counts_ref[...]
    mine = iota(counts.shape, 1) == lax.axis_index("pts")
    live_total = jnp.sum(jnp.where(mine, counts, 0), axis=1, keepdims=True)
    return span(lax.axis_index("bev")) * total + iota((1, total), 1) < live_total


def pool_part(span, hi_count, matrix, counts_ref, feats_ref, class_ref, band_ref, pillar_ref):
    feats = feats_ref[...]
    total = feats.shape[1]
    live = live_points(span, counts_ref, total)
    one_hot = to_f32(iota((16, total), 0) == class_ref[...])
    one_hot = jnp.where(iota((16, total), 0) == CLASSES, 1.0, one_hot)
    high, mid, low = split3(jnp.concatenate([feats, feats], axis=0))
    top = iota((8, total), 0) < 4
    first = jnp.where(top, high, mid)
    third = jnp.where(top, high, low)
    stacked = jnp.concatenate(
        [first, first, third, jnp.zeros_like(first), one_hot, one_hot, one_hot], axis=0
    ).astype(jnp.bfloat16)
    hidden = jnp.dot(matrix, stacked, preferred_element_type=jnp.float32)
    encoded = jnp.maximum(hidden, 0.0).astype(jnp.bfloat16)
    pillar = pillar_ref[...]
    hi = jnp.where(live & (band_ref[...] == lax.axis_index("bev")), pillar >> 8, 15)
    lo = pillar & (LO - 1)
    tall, lo_hot = two_level(encoded, hi, lo, hi_count)
    tall.append(to_f32(iota((16, total), 0) == hi).astype(jnp.bfloat16))
    return lax.dot_general(
        jnp.concatenate(tall, axis=0), lo_hot, NT, preferred_element_type=jnp.float32
    )


def order_pillars(pillars, sub_of, cell_ref, cell_pad, rank_ref, where_ref, starts_ref):
    hi_count = round_up(pillars, LO) // LO
    width = hi_count * LO
    cell_pad[...] = jnp.full(cell_pad.shape, -1, jnp.int32)
    cell_pad[:, :pillars] = cell_ref[...].reshape(1, pillars)
    cell = cell_pad[...]
    cell_f = cell.astype(jnp.float32)
    grid_row = jnp.floor((cell_f + 0.5) * (1.0 / COLS)).astype(jnp.int32)
    grid_col = cell - grid_row * COLS
    sub, lane = (grid_col, grid_row) if sub_of == "col" else (grid_row, grid_col)
    block = jnp.where(cell >= 0, sub >> 4, BUCKETS - 1)
    member = to_f32(iota((BUCKETS, width), 0) == block)
    before = to_f32(iota((LO, LO), 0) < iota((LO, LO), 1)).astype(jnp.bfloat16)
    offset = jnp.zeros((BUCKETS, 1), jnp.float32)
    ranks = []
    for h in range(hi_count):
        chunk = member[:, h * LO : (h + 1) * LO]
        prefix = jnp.dot(
            chunk.astype(jnp.bfloat16), before, preferred_element_type=jnp.float32
        )
        ranks.append(prefix + offset)
        offset = offset + jnp.sum(chunk, axis=1, keepdims=True)
    square = iota((BUCKETS, 128), 0)
    across = iota((BUCKETS, 128), 1)
    starts_row = jnp.sum(jnp.where(square < across, offset, 0.0), axis=0, keepdims=True)
    size_row = jnp.sum(jnp.where(square == across, offset, 0.0), axis=0, keepdims=True)
    starts_i = starts_row.astype(jnp.int32)
    reach = (starts_i & 127) + size_row.astype(jnp.int32)
    real = iota((1, 128), 1) < BUCKETS - 1
    wide = jnp.max(jnp.where(real, reach, 0), axis=1, keepdims=True) > LO
    starts_ref[...] = jnp.where(iota((1, 128), 1) == 127, wide.astype(jnp.int32), starts_i)
    start = jnp.sum(jnp.where(square == across, starts_row, 0.0), axis=1, keepdims=True)
    extra = iota((16, LO), 0)
    for h in range(hi_count):
        at = slice(h * LO, (h + 1) * LO)
        rank = jnp.sum(member[:, at] * (ranks[h] + start), axis=0, keepdims=True)
        rank_ref[:, at] = rank.astype(jnp.int32)
        sub_h = sub[:, at]
        lane_h = lane[:, at]
        where_ref[:, at] = jnp.where(
            extra == 0,
            block[:, at],
            jnp.where(
                extra == 1,
                sub_h & (STEP - 1),
                jnp.where(extra == 2, lane_h >> 8, jnp.where(extra == 3, lane_h & 255, 0)),
            ),
        ).astype(jnp.float32)


def first_body(
    span, spans, pillars, sub_of, counts_ref, scores_ref, weight_ref, bias_ref, cell_ref, *refs
):
    hi_count = round_up(pillars, LO) // LO
    own, other_classes = refs[:4], refs[4 : 4 + len(spans)]
    (
        sums_ref,
        matrix_ref,
        tally_ref,
        counts_out,
        rank_ref,
        where_ref,
        starts_ref,
        cell_pad,
    ) = refs[4 + len(spans) :]
    counts_out[...] = counts_ref[...]
    tally_ref[...] = class_tally([span, *spans], counts_ref, [own[1], *other_classes])
    matrix = encoder_matrix(weight_ref[...], scores_ref[...], bias_ref[...])
    matrix_ref[...] = matrix
    sums_ref[...] = pool_part(span, hi_count, matrix, counts_ref, *own)
    order_pillars(pillars, sub_of, cell_ref, cell_pad, rank_ref, where_ref, starts_ref)


def second_body(spans, pillars, counts_ref, matrix_ref, sums_in_ref, rank_ref, where_ref, *refs):
    parts = len(spans)
    (sorted_ref,) = refs[4 * parts :]
    channels = matrix_ref.shape[0]
    hi_count = round_up(pillars, LO) // LO
    sums = sums_in_ref[...]
    for part in range(parts):
        sums = sums + pool_part(
            spans[part], hi_count, matrix_ref[...], counts_ref, *refs[4 * part : 4 * part + 4]
        )

    placed = jnp.zeros((hi_count * (channels + 16), LO), jnp.float32)
    counts = sums[hi_count * channels :]
    for h in range(hi_count):
        at = slice(h * LO, (h + 1) * LO)
        rank = rank_ref[:, at]
        mean = sums[h * channels : (h + 1) * channels] / jnp.maximum(counts[h : h + 1], 1.0)
        values = jnp.concatenate([mean, where_ref[:, at]], axis=0).astype(jnp.bfloat16)
        tall, lo_hot = two_level(values, rank >> 8, rank & (LO - 1), hi_count)
        placed = placed + lax.dot_general(
            jnp.concatenate(tall, axis=0), lo_hot, NT, preferred_element_type=jnp.float32
        )
    rows = channels + 16
    tail = iota((8, LO), 0)
    for h in range(hi_count):
        piece = placed[h * rows : (h + 1) * rows]
        sub_s = piece[channels : channels + 1] * STEP + piece[channels + 1 : channels + 2]
        lane_s = piece[channels + 2 : channels + 3] * 256.0 + piece[channels + 3 : channels + 4]
        extra_s = jnp.where(tail == 0, sub_s, jnp.where(tail == 1, lane_s, 0.0))
        for half in range(2):
            at = slice(half * 128, half * 128 + 128)
            sorted_ref[2 * h + half, :channels, :] = piece[:channels, at]
            sorted_ref[2 * h + half, channels:, :] = extra_s[:, at]
    for chunk in range(2 * hi_count, 2 * hi_count + 2):
        sorted_ref[chunk, :channels, :] = jnp.zeros((channels, 128), jnp.float32)
        sorted_ref[chunk, channels:, :] = jnp.full((8, 128), -1.0, jnp.float32)


def place_body(starts_vmem, sorted_ref, out_ref, starts_ref, image, lane_hot, acc_ref, sem, sems):
    fetch = pltpu.make_async_copy(starts_vmem, starts_ref, sem)
    fetch.start()
    fetch.wait()
    channels, _, lanes = out_ref.shape
    chunks, wide, _ = lane_hot.shape
    blocks = image.shape[1] // STEP

    def hot_of(chunk):
        lane = sorted_ref[chunk, channels + 1 : channels + 2, :].astype(jnp.int32)
        return to_f32(iota((wide, 128), 0) == lane).astype(jnp.bfloat16)

    def base_of(block):
        return starts_ref[0, block] >> 7

    def partial(block, turn, ready=True):
        talls = []
        hots = []
        for half in range(2):
            chunk = base_of(block) + 2 * turn + half
            sub = sorted_ref[chunk, channels : channels + 1, :].astype(jnp.int32) - block * STEP
            mask_a = to_f32(iota((8, 128), 0) == sub)
            mask_b = to_f32(iota((8, 128), 0) + 8 == sub)
            tall = []
            for channel in range(channels):
                row = sorted_ref[chunk, pl.ds(channel, 8, stride=0), :]
                tall.append(
                    jnp.concatenate([row * mask_a, row * mask_b], axis=0).astype(jnp.bfloat16)
                )
            talls.append(jnp.concatenate(tall, axis=0))
            hots.append(lane_hot[chunk] if ready else hot_of(chunk))
        return lax.dot_general(
            jnp.concatenate(talls, axis=1),
            jnp.concatenate(hots, axis=1),
            NT,
            preferred_element_type=jnp.float32,
        )

    def put(block, value):
        rows = pl.ds(block * STEP, STEP)
        tile = value.astype(jnp.bfloat16).reshape(channels, STEP, wide)
        image[:, rows, :] = tile[:, :, :lanes]

    spans = []
    begin = 0
    while begin < blocks:
        end = min(begin + min(len(spans) + 1, GROUP), blocks)
        spans.append((begin, end))
        begin = end
    copies = []
    for index, (begin, end) in enumerate(spans):
        rows = pl.ds(begin * STEP, (end - begin) * STEP)
        copies.append(
            pltpu.make_async_copy(image.at[:, rows], out_ref.at[:, rows], sems.at[index])
        )
    spread = starts_ref[0, 127]

    @pl.when(spread == 0)
    def _():
        put(0, partial(0, 0, ready=False))
        copies[0].start()
        for chunk in range(chunks):
            lane_hot[chunk] = hot_of(chunk)
        for (begin, end), copy in zip(spans[1:], copies[1:]):
            for block in range(begin, end):
                put(block, partial(block, 0))
            copy.start()

    @pl.when(spread != 0)
    def _():
        @pl.loop(0, blocks)
        def _(block):
            turns = (starts_ref[0, block + 1] - base_of(block) * 128 + LO - 1) // LO
            acc_ref[...] = partial(block, 0, ready=False)

            @pl.loop(1, turns)
            def _(turn):
                acc_ref[...] += partial(block, turn, ready=False)

            put(pl.multiple_of(block, 1), acc_ref[...])

        for copy in copies:
            copy.start()

    for copy in copies:
        copy.wait()


def place(sorted_values, starts, channels, subs, lanes):
    wide = round_up(lanes, 128)
    blocks = pl.cdiv(subs, STEP)
    return pl.pallas_call(
        place_body,
        in_specs=[
            pl.BlockSpec(memory_space=pltpu.VMEM),
            pl.BlockSpec(memory_space=pltpu.VMEM),
        ],
        out_specs=pl.BlockSpec(memory_space=pl.ANY),
        scratch_shapes=[
            pltpu.SMEM((1, 128), jnp.int32),
            pltpu.VMEM((channels, blocks * STEP, lanes), jnp.bfloat16),
            pltpu.VMEM((sorted_values.shape[0], wide, 128), jnp.bfloat16),
            pltpu.VMEM((channels * STEP, wide), jnp.float32),
            pltpu.SemaphoreType.DMA,
            pltpu.SemaphoreType.DMA((blocks,)),
        ],
        out_shape=jax.ShapeDtypeStruct((channels, blocks * STEP, lanes), jnp.bfloat16),
        cost_estimate=pl.CostEstimate(flops=10**9, transcendentals=0, bytes_accessed=10**7),
        name="place",
    )(in_vmem(starts), in_vmem(sorted_values))[:, :subs]


def in_vmem(value):
    return pltpu.with_memory_space_constraint(value, pltpu.VMEM)


def all_tallies(total, frames, bands):
    stride = 1
    while stride < frames:
        radix = 4 if frames % (stride * 4) == 0 else 2
        received = []
        for hop in range(1, radix):
            pairs = [
                (i * bands + k, (i ^ (hop * stride)) * bands + bands - 1 - k)
                for i in range(frames)
                for k in range(bands)
            ]
            received.append(lax.ppermute(total, ("pts", "bev"), pairs))
        total = total + sum(received)
        stride *= radix
    return total


def on_device(
    point_feats,
    point_class,
    point_band,
    point_pillar,
    point_counts,
    pillar_cell,
    class_scores,
    encoder_weight,
    encoder_bias,
):
    band_count = lax.axis_size("bev")
    frames = lax.axis_size("pts")
    total = point_class.shape[0]
    pillars = pillar_cell.shape[-1]
    channels = encoder_weight.shape[0]
    band_rows = ROWS // band_count
    own = (
        point_feats,
        point_class.reshape(1, -1),
        point_band.reshape(1, -1),
        point_pillar.reshape(1, -1),
    )
    shifts = [
        [((i + shift) % band_count, i) for i in range(band_count)]
        for shift in range(1, band_count)
    ]
    other_classes = [in_vmem(lax.ppermute(own[1], "bev", pairs)) for pairs in shifts]
    others = []
    for pairs, classes in zip(shifts, other_classes):
        band, pillar, feats = [
            in_vmem(lax.ppermute(own[index], "bev", pairs)) for index in (2, 3, 0)
        ]
        others.extend((feats, classes, band, pillar))
    spans = [lambda band, k=k: (band + k) % band_count for k in range(1, band_count)]

    def own_span(band):
        return band

    def tiles(subs, lanes):
        return round_up(subs, 16) * round_up(lanes, 128)

    sub_of = "col" if tiles(COLS, band_rows) <= tiles(band_rows, COLS) else "row"
    subs, lanes = (COLS, band_rows) if sub_of == "col" else (band_rows, COLS)
    width = round_up(pillars, LO)
    vmem = pl.BlockSpec(memory_space=pltpu.VMEM)
    hi_count = width // LO
    sums, matrix, tally, counts, rank, where, starts = pl.pallas_call(
        lambda *refs: first_body(own_span, spans, pillars, sub_of, *refs),
        in_specs=[vmem] * (9 + len(other_classes)),
        out_specs=(vmem,) * 7,
        out_shape=(
            pltpu.VMEM((hi_count * channels + 16, LO), jnp.float32),
            pltpu.VMEM((channels, 80), jnp.bfloat16),
            pltpu.VMEM((1, 128), jnp.float32),
            pltpu.VMEM((1, frames), jnp.int32),
            pltpu.VMEM((1, width), jnp.int32),
            pltpu.VMEM((16, width), jnp.float32),
            pltpu.VMEM((1, 128), jnp.int32),
        ),
        scratch_shapes=[pltpu.VMEM((1, width), jnp.int32)],
        cost_estimate=pl.CostEstimate(flops=10**9, transcendentals=0, bytes_accessed=10**6),
        name="pool_own",
    )(
        point_counts.reshape(1, frames),
        class_scores,
        encoder_weight.T,
        encoder_bias.reshape(1, channels),
        pillar_cell.reshape(1, pillars),
        *own,
        *other_classes,
    )
    class_counts = (all_tallies(tally, frames, band_count) / total)[0, :CLASSES]
    sorted_values = pl.pallas_call(
        lambda *refs: second_body(spans, pillars, *refs),
        in_specs=[vmem] * (5 + len(others)),
        out_specs=vmem,
        out_shape=pltpu.VMEM(((width + LO) // 128, channels + 8, 128), jnp.float32),
        cost_estimate=pl.CostEstimate(flops=10**9, transcendentals=0, bytes_accessed=10**6),
        name="pool_rest",
    )(*[in_vmem(x) for x in (counts, matrix, sums, rank, where)], *others)
    planes = place(sorted_values, starts, channels, subs, lanes)
    bev_image = planes.swapaxes(1, 2) if sub_of == "col" else planes
    return (bev_image[None], class_counts)


def solution(mesh):
    return jax.shard_map(
        on_device,
        mesh=mesh,
        in_specs=(
            P(None, ("pts", "bev")),
            P(("pts", "bev")),
            P(("pts", "bev")),
            P(("pts", "bev")),
            P(),
            P("pts", "bev", None),
            P(),
            P(),
            P(),
        ),
        out_specs=(P("pts", None, "bev", None), P()),
        check_vma=False,
    )
```

```python
import jax
import jax.numpy as jnp
from jax import lax
from jax.experimental import pallas as pl
from jax.experimental.pallas import tpu as pltpu
from jax.sharding import PartitionSpec as P

ROWS = 496
COLS = 432
CLASSES = 11

LO = 256
STEP = 16
BUCKETS = 32
GROUP = 3
HIGHEST = lax.Precision.HIGHEST
NT = (((1,), (1,)), ((), ()))


def round_up(value, unit):
    return -(-value // unit) * unit


def iota(shape, axis):
    return lax.broadcasted_iota(jnp.int32, shape, axis)


def to_f32(mask):
    return jnp.where(mask, 1.0, 0.0).astype(jnp.float32)


def split3(value):
    high = value.astype(jnp.bfloat16).astype(jnp.float32)
    rest = value - high
    mid = rest.astype(jnp.bfloat16).astype(jnp.float32)
    return high, mid, rest - mid


def encoder_matrix(weight_t, scores, bias_row):
    columns, channels = weight_t.shape
    lane = iota((columns, 80), 1)
    row = iota((columns, 80), 0)
    pick = to_f32((lane < 24) & ((lane & 3) == row))
    shift = to_f32(iota((columns, CLASSES), 0) == iota((columns, CLASSES), 1) + 4)
    place_lane = iota((CLASSES, 80), 1)
    place = to_f32((place_lane >= 32) & ((place_lane & 15) == iota((CLASSES, 80), 0)))
    spread = jnp.dot(
        jnp.dot(shift, scores, precision=HIGHEST, preferred_element_type=jnp.float32),
        place,
        precision=HIGHEST,
        preferred_element_type=jnp.float32,
    )
    matrix = lax.dot_general(
        weight_t,
        pick + spread,
        (((0,), (0,)), ((), ())),
        precision=HIGHEST,
        preferred_element_type=jnp.float32,
    )
    eye = iota((channels, channels), 0) == iota((channels, channels), 1)
    bias = jnp.sum(jnp.where(eye, bias_row, 0.0), axis=1, keepdims=True)
    out_lane = iota((channels, 80), 1)
    matrix = matrix + jnp.where((out_lane >= 32) & ((out_lane & 15) == CLASSES), bias, 0.0)
    high, mid, low = split3(matrix)
    take_mid = ((out_lane >= 8) & (out_lane < 16)) | ((out_lane >= 48) & (out_lane < 64))
    take_low = ((out_lane >= 16) & (out_lane < 20)) | (out_lane >= 64)
    return jnp.where(take_mid, mid, jnp.where(take_low, low, high)).astype(jnp.bfloat16)


def two_level(values, hi, lo, hi_count):
    _, total = values.shape
    tall = [values * to_f32(hi == h).astype(jnp.bfloat16) for h in range(hi_count)]
    one_hot = to_f32(iota((LO, total), 0) == lo).astype(jnp.bfloat16)
    return tall, one_hot


def class_tally(spans, counts_ref, class_refs):
    tally = jnp.zeros((16, 128), jnp.float32)
    for span, class_ref in zip(spans, class_refs):
        classes = class_ref[...]
        total = classes.shape[1]
        live = live_points(span, counts_ref, total)
        one_hot = to_f32((iota((16, total), 0) == classes) & live)
        for begin in range(0, total, 128):
            tally = tally + one_hot[:, begin : begin + 128]
    tally = jnp.sum(tally, axis=1, keepdims=True)
    diagonal = iota((16, 128), 0) == iota((16, 128), 1)
    return jnp.sum(jnp.where(diagonal, tally, 0.0), axis=0, keepdims=True)


def live_points(span, counts_ref, total):
    counts = counts_ref[...]
    mine = iota(counts.shape, 1) == lax.axis_index("pts")
    live_total = jnp.sum(jnp.where(mine, counts, 0), axis=1, keepdims=True)
    return span(lax.axis_index("bev")) * total + iota((1, total), 1) < live_total


def pool_part(span, hi_count, matrix, counts_ref, feats_ref, class_ref, band_ref, pillar_ref):
    feats = feats_ref[...]
    total = feats.shape[1]
    live = live_points(span, counts_ref, total)
    one_hot = to_f32(iota((16, total), 0) == class_ref[...])
    one_hot = jnp.where(iota((16, total), 0) == CLASSES, 1.0, one_hot)
    high, mid, low = split3(jnp.concatenate([feats, feats], axis=0))
    top = iota((8, total), 0) < 4
    first = jnp.where(top, high, mid)
    third = jnp.where(top, high, low)
    stacked = jnp.concatenate(
        [first, first, third, jnp.zeros_like(first), one_hot, one_hot, one_hot], axis=0
    ).astype(jnp.bfloat16)
    hidden = jnp.dot(matrix, stacked, preferred_element_type=jnp.float32)
    encoded = jnp.maximum(hidden, 0.0).astype(jnp.bfloat16)
    pillar = pillar_ref[...]
    hi = jnp.where(live & (band_ref[...] == lax.axis_index("bev")), pillar >> 8, 15)
    lo = pillar & (LO - 1)
    tall, lo_hot = two_level(encoded, hi, lo, hi_count)
    tall.append(to_f32(iota((16, total), 0) == hi).astype(jnp.bfloat16))
    return lax.dot_general(
        jnp.concatenate(tall, axis=0), lo_hot, NT, preferred_element_type=jnp.float32
    )


def order_pillars(pillars, sub_of, cell_ref, cell_pad, rank_ref, where_ref, starts_ref):
    hi_count = round_up(pillars, LO) // LO
    width = hi_count * LO
    cell_pad[...] = jnp.full(cell_pad.shape, -1, jnp.int32)
    cell_pad[:, :pillars] = cell_ref[...].reshape(1, pillars)
    cell = cell_pad[...]
    cell_f = cell.astype(jnp.float32)
    grid_row = jnp.floor((cell_f + 0.5) * (1.0 / COLS)).astype(jnp.int32)
    grid_col = cell - grid_row * COLS
    sub, lane = (grid_col, grid_row) if sub_of == "col" else (grid_row, grid_col)
    block = jnp.where(cell >= 0, sub >> 4, BUCKETS - 1)
    member = to_f32(iota((BUCKETS, width), 0) == block)
    before = to_f32(iota((LO, LO), 0) < iota((LO, LO), 1)).astype(jnp.bfloat16)
    offset = jnp.zeros((BUCKETS, 1), jnp.float32)
    ranks = []
    for h in range(hi_count):
        chunk = member[:, h * LO : (h + 1) * LO]
        prefix = jnp.dot(
            chunk.astype(jnp.bfloat16), before, preferred_element_type=jnp.float32
        )
        ranks.append(prefix + offset)
        offset = offset + jnp.sum(chunk, axis=1, keepdims=True)
    square = iota((BUCKETS, 128), 0)
    across = iota((BUCKETS, 128), 1)
    starts_row = jnp.sum(jnp.where(square < across, offset, 0.0), axis=0, keepdims=True)
    size_row = jnp.sum(jnp.where(square == across, offset, 0.0), axis=0, keepdims=True)
    starts_i = starts_row.astype(jnp.int32)
    reach = (starts_i & 127) + size_row.astype(jnp.int32)
    real = iota((1, 128), 1) < BUCKETS - 1
    wide = jnp.max(jnp.where(real, reach, 0), axis=1, keepdims=True) > LO
    starts_ref[...] = jnp.where(iota((1, 128), 1) == 127, wide.astype(jnp.int32), starts_i)
    start = jnp.sum(jnp.where(square == across, starts_row, 0.0), axis=1, keepdims=True)
    extra = iota((16, LO), 0)
    for h in range(hi_count):
        at = slice(h * LO, (h + 1) * LO)
        rank = jnp.sum(member[:, at] * (ranks[h] + start), axis=0, keepdims=True)
        rank_ref[:, at] = rank.astype(jnp.int32)
        sub_h = sub[:, at]
        lane_h = lane[:, at]
        where_ref[:, at] = jnp.where(
            extra == 0,
            block[:, at],
            jnp.where(
                extra == 1,
                sub_h & (STEP - 1),
                jnp.where(extra == 2, lane_h >> 8, jnp.where(extra == 3, lane_h & 255, 0)),
            ),
        ).astype(jnp.float32)


def first_body(
    span, spans, pillars, sub_of, counts_ref, scores_ref, weight_ref, bias_ref, cell_ref, *refs
):
    hi_count = round_up(pillars, LO) // LO
    own, other_classes = refs[:4], refs[4 : 4 + len(spans)]
    (
        sums_ref,
        matrix_ref,
        tally_ref,
        counts_out,
        rank_ref,
        where_ref,
        starts_ref,
        cell_pad,
    ) = refs[4 + len(spans) :]
    counts_out[...] = counts_ref[...]
    tally_ref[...] = class_tally([span, *spans], counts_ref, [own[1], *other_classes])
    matrix = encoder_matrix(weight_ref[...], scores_ref[...], bias_ref[...])
    matrix_ref[...] = matrix
    sums_ref[...] = pool_part(span, hi_count, matrix, counts_ref, *own)
    order_pillars(pillars, sub_of, cell_ref, cell_pad, rank_ref, where_ref, starts_ref)


def second_body(
    spans, pillars, counts_ref, matrix_ref, sums_in_ref, rank_ref, where_ref, starts_ref, *refs
):
    parts = len(spans)
    sorted_ref, starts_smem, sem = refs[4 * parts :]
    move = pltpu.make_async_copy(starts_ref, starts_smem, sem)
    move.start()
    channels = matrix_ref.shape[0]
    hi_count = round_up(pillars, LO) // LO
    sums = sums_in_ref[...]
    for part in range(parts):
        sums = sums + pool_part(
            spans[part], hi_count, matrix_ref[...], counts_ref, *refs[4 * part : 4 * part + 4]
        )

    placed = jnp.zeros((hi_count * (channels + 16), LO), jnp.float32)
    counts = sums[hi_count * channels :]
    for h in range(hi_count):
        at = slice(h * LO, (h + 1) * LO)
        rank = rank_ref[:, at]
        mean = sums[h * channels : (h + 1) * channels] / jnp.maximum(counts[h : h + 1], 1.0)
        values = jnp.concatenate([mean, where_ref[:, at]], axis=0).astype(jnp.bfloat16)
        tall, lo_hot = two_level(values, rank >> 8, rank & (LO - 1), hi_count)
        placed = placed + lax.dot_general(
            jnp.concatenate(tall, axis=0), lo_hot, NT, preferred_element_type=jnp.float32
        )
    rows = channels + 16
    tail = iota((8, LO), 0)
    for h in range(hi_count):
        piece = placed[h * rows : (h + 1) * rows]
        sub_s = piece[channels : channels + 1] * STEP + piece[channels + 1 : channels + 2]
        lane_s = piece[channels + 2 : channels + 3] * 256.0 + piece[channels + 3 : channels + 4]
        extra_s = jnp.where(tail == 0, sub_s, jnp.where(tail == 1, lane_s, 0.0))
        for half in range(2):
            at = slice(half * 128, half * 128 + 128)
            sorted_ref[2 * h + half, :channels, :] = piece[:channels, at]
            sorted_ref[2 * h + half, channels:, :] = extra_s[:, at]
    for chunk in range(2 * hi_count, 2 * hi_count + 2):
        sorted_ref[chunk, :channels, :] = jnp.zeros((channels, 128), jnp.float32)
        sorted_ref[chunk, channels:, :] = jnp.full((8, 128), -1.0, jnp.float32)
    move.wait()


def place_body(starts_ref, sorted_ref, out_ref, image, acc_ref, sems):
    channels, _, lanes = out_ref.shape
    wide = acc_ref.shape[1]
    blocks = image.shape[1] // STEP

    def hot_of(chunk):
        lane = sorted_ref[chunk, channels + 1 : channels + 2, :].astype(jnp.int32)
        return to_f32(iota((wide, 128), 0) == lane).astype(jnp.bfloat16)

    def base_of(block):
        return starts_ref[0, block] >> 7

    def partial(block, turn):
        talls = []
        hots = []
        for half in range(2):
            chunk = base_of(block) + 2 * turn + half
            sub = sorted_ref[chunk, channels : channels + 1, :].astype(jnp.int32) - block * STEP
            mask_a = to_f32(iota((8, 128), 0) == sub)
            mask_b = to_f32(iota((8, 128), 0) + 8 == sub)
            tall = []
            for channel in range(channels):
                row = sorted_ref[chunk, pl.ds(channel, 8, stride=0), :]
                tall.append(
                    jnp.concatenate([row * mask_a, row * mask_b], axis=0).astype(jnp.bfloat16)
                )
            talls.append(jnp.concatenate(tall, axis=0))
            hots.append(hot_of(chunk))
        return lax.dot_general(
            jnp.concatenate(talls, axis=1),
            jnp.concatenate(hots, axis=1),
            NT,
            preferred_element_type=jnp.float32,
        )

    def put(block, value):
        rows = pl.ds(block * STEP, STEP)
        tile = value.astype(jnp.bfloat16).reshape(channels, STEP, wide)
        image[:, rows, :] = tile[:, :, :lanes]

    spans = []
    begin = 0
    while begin < blocks:
        end = min(begin + min(len(spans) // 2 + 1, GROUP), blocks)
        spans.append((begin, end))
        begin = end
    copies = []
    for index, (begin, end) in enumerate(spans):
        rows = pl.ds(begin * STEP, (end - begin) * STEP)
        copies.append(
            pltpu.make_async_copy(image.at[:, rows], out_ref.at[:, rows], sems.at[index])
        )
    spread = starts_ref[0, 127]

    @pl.when(spread == 0)
    def _():
        for (begin, end), copy in zip(spans, copies):
            for block in range(begin, end):
                put(block, partial(block, 0))
            copy.start()

    @pl.when(spread != 0)
    def _():
        @pl.loop(0, blocks)
        def _(block):
            turns = (starts_ref[0, block + 1] - base_of(block) * 128 + LO - 1) // LO
            acc_ref[...] = partial(block, 0)

            @pl.loop(1, turns)
            def _(turn):
                acc_ref[...] += partial(block, turn)

            put(pl.multiple_of(block, 1), acc_ref[...])

        for copy in copies:
            copy.start()

    for copy in copies:
        copy.wait()


def place(sorted_values, starts, channels, subs, lanes):
    wide = round_up(lanes, 128)
    blocks = pl.cdiv(subs, STEP)
    return pl.pallas_call(
        place_body,
        in_specs=[
            pl.BlockSpec(memory_space=pltpu.SMEM),
            pl.BlockSpec(memory_space=pltpu.VMEM),
        ],
        out_specs=pl.BlockSpec(memory_space=pl.ANY),
        scratch_shapes=[
            pltpu.VMEM((channels, blocks * STEP, lanes), jnp.bfloat16),
            pltpu.VMEM((channels * STEP, wide), jnp.float32),
            pltpu.SemaphoreType.DMA((blocks,)),
        ],
        out_shape=jax.ShapeDtypeStruct((channels, blocks * STEP, lanes), jnp.bfloat16),
        cost_estimate=pl.CostEstimate(flops=10**9, transcendentals=0, bytes_accessed=10**7),
        name="place",
    )(pltpu.with_memory_space_constraint(starts, pltpu.SMEM), in_vmem(sorted_values))[:, :subs]


def in_vmem(value):
    return pltpu.with_memory_space_constraint(value, pltpu.VMEM)


def all_tallies(total, frames, bands):
    stride = 1
    while stride < frames:
        radix = 4 if frames % (stride * 4) == 0 else 2
        received = []
        for hop in range(1, radix):
            pairs = [
                (i * bands + k, (i ^ (hop * stride)) * bands + bands - 1 - k)
                for i in range(frames)
                for k in range(bands)
            ]
            received.append(lax.ppermute(total, ("pts", "bev"), pairs))
        total = total + sum(received)
        stride *= radix
    return total


def on_device(
    point_feats,
    point_class,
    point_band,
    point_pillar,
    point_counts,
    pillar_cell,
    class_scores,
    encoder_weight,
    encoder_bias,
):
    band_count = lax.axis_size("bev")
    frames = lax.axis_size("pts")
    total = point_class.shape[0]
    pillars = pillar_cell.shape[-1]
    channels = encoder_weight.shape[0]
    band_rows = ROWS // band_count
    own = (
        point_feats,
        point_class.reshape(1, -1),
        point_band.reshape(1, -1),
        point_pillar.reshape(1, -1),
    )
    shifts = [
        [((i + shift) % band_count, i) for i in range(band_count)]
        for shift in range(1, band_count)
    ]
    other_classes = [in_vmem(lax.ppermute(own[1], "bev", pairs)) for pairs in shifts]
    others = []
    for pairs, classes in zip(shifts, other_classes):
        band, pillar, feats = [
            in_vmem(lax.ppermute(own[index], "bev", pairs)) for index in (2, 3, 0)
        ]
        others.extend((feats, classes, band, pillar))
    spans = [lambda band, k=k: (band + k) % band_count for k in range(1, band_count)]

    def own_span(band):
        return band

    def tiles(subs, lanes):
        return round_up(subs, 16) * round_up(lanes, 128)

    sub_of = "col" if tiles(COLS, band_rows) <= tiles(band_rows, COLS) else "row"
    subs, lanes = (COLS, band_rows) if sub_of == "col" else (band_rows, COLS)
    width = round_up(pillars, LO)
    vmem = pl.BlockSpec(memory_space=pltpu.VMEM)
    hi_count = width // LO
    sums, matrix, tally, counts, rank, where, starts = pl.pallas_call(
        lambda *refs: first_body(own_span, spans, pillars, sub_of, *refs),
        in_specs=[vmem] * (9 + len(other_classes)),
        out_specs=(vmem,) * 7,
        out_shape=(
            pltpu.VMEM((hi_count * channels + 16, LO), jnp.float32),
            pltpu.VMEM((channels, 80), jnp.bfloat16),
            pltpu.VMEM((1, 128), jnp.float32),
            pltpu.VMEM((1, frames), jnp.int32),
            pltpu.VMEM((1, width), jnp.int32),
            pltpu.VMEM((16, width), jnp.float32),
            pltpu.VMEM((1, 128), jnp.int32),
        ),
        scratch_shapes=[pltpu.VMEM((1, width), jnp.int32)],
        cost_estimate=pl.CostEstimate(flops=10**9, transcendentals=0, bytes_accessed=10**6),
        name="pool_own",
    )(
        point_counts.reshape(1, frames),
        class_scores,
        encoder_weight.T,
        encoder_bias.reshape(1, channels),
        pillar_cell.reshape(1, pillars),
        *own,
        *other_classes,
    )
    class_counts = (all_tallies(tally, frames, band_count) / total)[0, :CLASSES]
    sorted_values, starts = pl.pallas_call(
        lambda *refs: second_body(spans, pillars, *refs),
        in_specs=[vmem] * (6 + len(others)),
        out_specs=(vmem, pl.BlockSpec(memory_space=pltpu.SMEM)),
        out_shape=(
            pltpu.VMEM(((width + LO) // 128, channels + 8, 128), jnp.float32),
            pltpu.SMEM((1, 128), jnp.int32),
        ),
        scratch_shapes=[pltpu.SemaphoreType.DMA],
        cost_estimate=pl.CostEstimate(flops=10**9, transcendentals=0, bytes_accessed=10**6),
        name="pool_rest",
    )(*[in_vmem(x) for x in (counts, matrix, sums, rank, where, starts)], *others)
    planes = place(sorted_values, starts, channels, subs, lanes)
    bev_image = planes.swapaxes(1, 2) if sub_of == "col" else planes
    return (bev_image[None], class_counts)


def solution(mesh):
    return jax.shard_map(
        on_device,
        mesh=mesh,
        in_specs=(
            P(None, ("pts", "bev")),
            P(("pts", "bev")),
            P(("pts", "bev")),
            P(("pts", "bev")),
            P(),
            P("pts", "bev", None),
            P(),
            P(),
            P(),
        ),
        out_specs=(P("pts", None, "bev", None), P()),
        check_vma=False,
    )
```
